32 devices in a mesh: section: 4 (over z), rep: 8 (over y, x, core).
Axes of the slice: x: 2, y: 2, z: 4, core: 2. Of those that a mesh axis runs over, the one named last changes fastest.
Arguments:
- cache: bfloat16 [4, 4096, 3584], P('section', 'rep'), may hold values from -6 to 6
- payload: bfloat16 [4, 4096, 3584], P('section', 'rep'), may hold values from -6 to 6
- block_ids: int32 [4, 8, 2], P('section', 'rep'), may hold values from 0 to 3, as said below
- block_counts: int32 [4, 8], P('section', 'rep'), may hold values from 1 to 2, as said below
- block_scales: int32 [4, 8, 2], P('section', 'rep'), may hold values from 1024 to 8192
- refresh_ids: int32 [4, 8, 128], P('section', 'rep'), may hold values from 0 to 511, as said below
- refresh_counts: int32 [4, 8], P('section', 'rep'), may hold values from 1 to 128, as said below
- norm_gain: float32 [4, 3584], P('section'), may hold values from 0.5 to 1.5
- query_weight: bfloat16 [4, 3584, 3584], P('section', 'rep'), may hold values from -0.09375 to 0.09375
- query_bias: float32 [4, 3584], P('section'), may hold values from -3 to 3
- kv_weight: bfloat16 [4, 3584, 1024], P('section', 'rep'), may hold values from -0.09375 to 0.09375
- kv_bias: float32 [4, 1024], P('section'), may hold values from -3 to 3
Outputs:
- rebuilt: bfloat16 [4, 4096, 3584], P('section', 'rep')
- queries: bfloat16 [4, 4096, 3584], P('section', 'rep')
- keys_values: bfloat16 [4, 4096, 1024], P('section', 'rep')
The draws below stay inside these ranges and needn't reach their ends.
Inputs may be any that keep to these rules, and one draw needn't show every extreme that they name: `block_ids`: for each section and relay the 2 entries are different block numbers; only the first block_counts entries are used. `block_counts`: in every section some relay lists exactly 2 blocks. `refresh_ids`: for each section and relay the entries are different local row numbers; only the first refresh_counts entries are used. `refresh_counts`: in every section some relay lists exactly 128 rows.
All inputs are finite; a program needn't handle non-finite values.
Results may differ from the reference program's by a relative error of at most 0.0052.
Values may be sent and summed in bfloat16 or wider, within the bound.
A program may use at most 256 MiB of HBM per device.

```python
import jax
import jax.numpy as jnp
from jax import lax

D = 3584
QW = 3584
KVW = 1024
BLK = 128
NBLK = 4
MOST_BLK = 2
REF_MAX = 128
ROW_DEV = 512
REPS = 8
SECTIONS = 4
ROWS = 4096


def pick_distinct(key, extent, amount):
    key_list = jax.random.split(key, SECTIONS * REPS)
    chosen = jax.vmap(lambda single: jax.random.permutation(single, extent)[:amount])(key_list)
    return chosen.reshape(SECTIONS, REPS, amount).astype(jnp.int32)


def counts_reaching(key, ceiling):
    front_key, place_key = jax.random.split(key)
    counts = jax.random.randint(front_key, (SECTIONS, REPS), 1, ceiling + 1)
    full_rank = jax.random.randint(place_key, (SECTIONS,), 0, REPS)
    at_full = jnp.arange(REPS)[None, :] == full_rank[:, None]
    return jnp.where(at_full, ceiling, counts).astype(jnp.int32)


def draw_block_ids(key, part):
    return pick_distinct(jax.random.fold_in(key, 11), NBLK, MOST_BLK)


def draw_block_counts(key, part):
    return counts_reaching(jax.random.fold_in(key, 12), MOST_BLK)


def draw_refresh_ids(key, part):
    return pick_distinct(jax.random.fold_in(key, 13), ROW_DEV, REF_MAX)


def draw_refresh_counts(key, part):
    return counts_reaching(jax.random.fold_in(key, 14), REF_MAX)


def touch_ends(values, own_key, low, largest):
    longest = values.shape.index(max(values.shape))
    spots = []
    for shift in (0, 1):
        where = [jax.random.randint(jax.random.fold_in(own_key, axis), (), 0, length) for axis, length in enumerate(values.shape)]
        where[longest] = (where[longest] + shift) % values.shape[longest]
        spots.append(tuple(where))
    return values.at[spots[0]].set(low).at[spots[1]].set(largest)


def level_of(stream_key, dims, pieces, smallest, largest):
    def one(axis_at, blocks):
        heights = jax.random.uniform(jax.random.fold_in(jax.random.fold_in(stream_key, 6), axis_at), (blocks,), jnp.float32, smallest / len(pieces), largest / len(pieces))
        return jnp.repeat(jnp.exp(heights), dims[axis_at] // blocks).reshape((-1,) + (1,) * (len(dims) - axis_at - 1))

    level = one(*pieces[0])
    for cut in pieces[1:]:
        level = level * one(*cut)
    return level


def scatter_about(rng, dims, deviation, bound, cuts=(), kind=jnp.bfloat16):
    entries = deviation * jax.random.normal(rng, dims, jnp.float32)
    if cuts:
        entries = entries * level_of(rng, dims, cuts, -0.22, 0.18)
    return jnp.clip(entries, -bound, bound).astype(kind)


def setup_inputs(seed: int = 0) -> dict:
    keys = jax.random.split(jax.random.key(seed), 13)
    return {
        "cache": scatter_about(keys[0], (SECTIONS, ROWS, D), 1.0, 6.0, ((0, 4), (1, 8))),
        "payload": scatter_about(keys[1], (SECTIONS, ROWS, D), 1.0, 6.0, ((0, 4), (1, 8))),
        "block_ids": draw_block_ids(jax.random.fold_in(keys[12], 71), 0),
        "block_counts": draw_block_counts(jax.random.fold_in(keys[12], 71), 0),
        "block_scales": touch_ends(jax.random.randint(keys[4], (SECTIONS, REPS, MOST_BLK), 1024, 8193), jax.random.fold_in(keys[4], 1), 1024, 8192).astype(jnp.int32),
        "refresh_ids": draw_refresh_ids(jax.random.fold_in(keys[12], 71), 0),
        "refresh_counts": draw_refresh_counts(jax.random.fold_in(keys[12], 71), 0),
        "norm_gain": jnp.clip(1.0 + 0.1 * jax.random.normal(keys[7], (SECTIONS, D), jnp.float32), 0.5, 1.5),
        "query_weight": scatter_about(keys[8], (SECTIONS, D, QW), D ** -0.5, 0.09375, ((0, 4), (1, 8))),
        "query_bias": scatter_about(keys[9], (SECTIONS, QW), 0.5, 3.0, ((0, 4),), jnp.float32),
        "kv_weight": scatter_about(keys[10], (SECTIONS, D, KVW), D ** -0.5, 0.09375, ((0, 4), (1, 8))),
        "kv_bias": scatter_about(keys[11], (SECTIONS, KVW), 0.5, 3.0, ((0, 4),), jnp.float32),
    }


def rebuild(stored, sent, ids, counts, scales, rows_sent, rows_counts):
    stored_blocks = stored.reshape(REPS, NBLK, BLK, D).astype(jnp.float32)
    sent_blocks = sent.reshape(REPS, NBLK, BLK, D).astype(jnp.float32)
    live = jnp.arange(MOST_BLK)[None, :] < counts[:, None]
    factor = jnp.where(live, scales.astype(jnp.float32) / 4096.0, 0.0)
    select = (ids[:, :, None] == jnp.arange(NBLK)[None, None, :]).astype(jnp.float32)
    per_block = lax.optimization_barrier(jnp.sum(factor[:, :, None] * select, axis=1))
    delta = (sent_blocks * per_block[:, :, None, None]).astype(jnp.bfloat16)
    delta = lax.optimization_barrier(delta).astype(jnp.float32)
    mixed = (stored_blocks + delta).reshape(REPS, ROW_DEV, D)
    live_rows = jnp.arange(REF_MAX)[None, :] < rows_counts[:, None]
    matches = (rows_sent[:, :, None] == jnp.arange(ROW_DEV)[None, None, :]) & live_rows[:, :, None]
    hit = jnp.any(matches, axis=1)
    mixed = jnp.where(hit[:, :, None], sent_blocks.reshape(REPS, ROW_DEV, D), mixed)
    return mixed.reshape(REPS * ROW_DEV, D).astype(jnp.bfloat16)

def project(rebuilt_section, gain, query_weight, query_bias, kv_weight, kv_bias):
    wide = rebuilt_section.astype(jnp.float32)
    scale_rows = lax.rsqrt(lax.optimization_barrier(jnp.mean(wide * wide, axis=1, keepdims=True)) + 1e-06)
    normed = (wide * scale_rows * gain[None, :]).astype(jnp.bfloat16)
    queries = jnp.dot(normed, query_weight, preferred_element_type=jnp.float32) + query_bias[None, :]
    keys_values = jnp.dot(normed, kv_weight, preferred_element_type=jnp.float32) + kv_bias[None, :]
    return (queries.astype(jnp.bfloat16), keys_values.astype(jnp.bfloat16))

def reference(cache, payload, block_ids, block_counts, block_scales, refresh_ids, refresh_counts, norm_gain, query_weight, query_bias, kv_weight, kv_bias):
    rebuilt_list = []
    query_list = []
    kv_list = []
    for section in range(SECTIONS):
        if section == 0:
            rebuilt_section = cache[0]
        else:
            rebuilt_section = rebuild(cache[section], payload[section - 1], block_ids[section - 1], block_counts[section - 1], block_scales[section - 1], refresh_ids[section - 1], refresh_counts[section - 1])
        queries, keys_values = project(rebuilt_section, norm_gain[section], query_weight[section], query_bias[section], kv_weight[section], kv_bias[section])
        rebuilt_list.append(rebuilt_section)
        query_list.append(queries)
        kv_list.append(keys_values)
    return (jnp.stack(rebuilt_list), jnp.stack(query_list), jnp.stack(kv_list))
```

```python
import functools

import jax
import jax.numpy as jnp
from jax import lax
from jax.experimental import pallas as pl
from jax.experimental.pallas import tpu as pltpu
from jax.sharding import PartitionSpec as P

BLK = 128
CW = 256
TILE = 16
EPSILON = 1e-06
MESH = pl.DeviceIdType.MESH


def chip_at(pos, chips):
    half = chips // 2
    back = pos // half
    return pos + back * (half + chips - 1 - 2 * pos)


def kernel(
    sections,
    reps,
    most_blk,
    meta_ref,
    payload_ref,
    cache_ref,
    gain_ref,
    qw_ref,
    qb_ref,
    kvw_ref,
    kvb_ref,
    rebuilt_ref,
    q_ref,
    kv_ref,
    w,
    values,
    stored,
    normed,
    staged,
    bias,
    meta,
    local_sem,
    keep_sem,
    row_send,
    row_recv,
    own_send,
    pair_own_recv,
    ring_send,
    ring_recv,
    pair_send,
    pair_recv,
    out_sem,
):
    chips = reps // 2
    hops = chips // 2
    depth = qw_ref.shape[1]
    rows = payload_ref.shape[1]
    feature = payload_ref.shape[2]
    nq = qw_ref.shape[2] // CW
    nc = nq + kvw_ref.shape[2] // CW
    nh = nc // 2
    row_chunks = rows // BLK

    section = lax.axis_index("section")
    me = lax.axis_index("rep")
    core = me % 2
    chip = me // 2
    pos = chip + (chip // hops) * (hops + chips - 1 - 2 * chip)
    partner = 2 * chip + (1 - core)

    def rep_at(place, which):
        return 2 * chip_at((place + chips) % chips, chips) + which

    towards = (rep_at(pos + 1, core), rep_at(pos - 1, core))

    barrier = pltpu.get_barrier_semaphore()
    for other in (partner,) + towards:
        pl.semaphore_signal(barrier, 1, device_id={"rep": other}, device_id_type=MESH)

    @pl.when(section > 0)
    def _():
        pl.semaphore_signal(
            barrier, 1, device_id={"section": section - 1}, device_id_type=MESH
        )

    @pl.when(section < sections - 1)
    def _():
        pl.semaphore_signal(
            barrier, 1, device_id={"section": section + 1}, device_id_type=MESH
        )

    def own(c):
        if c < nq:
            return qw_ref.at[0, :, pl.ds(c * CW, CW)]
        return kvw_ref.at[0, :, pl.ds((c - nq) * CW, CW)]

    def slot(c, block):
        return w.at[c, pl.ds(pl.multiple_of(block * depth, depth), depth), :]

    keep = pltpu.make_async_copy(cache_ref.at[0], stored, keep_sem)
    keep.start()
    own_locals = [
        pltpu.make_async_copy(own(c), slot(c, me), local_sem.at[c]) for c in range(nc)
    ]

    sides = (section + sections - 1) // sections + (2 * sections - 2 - section) // sections
    pl.semaphore_wait(barrier, 3 + sides)

    def meta_copy():
        return pltpu.make_async_remote_copy(
            src_ref=meta_ref,
            dst_ref=meta,
            send_sem=row_send.at[row_chunks],
            recv_sem=row_recv.at[row_chunks],
            device_id={"section": section + 1},
            device_id_type=MESH,
        )

    def row_copy(j):
        return pltpu.make_async_remote_copy(
            src_ref=payload_ref.at[0, pl.ds(j * BLK, BLK), :],
            dst_ref=values.at[pl.ds(j * BLK, BLK), :],
            send_sem=row_send.at[j],
            recv_sem=row_recv.at[j],
            device_id={"section": section + 1},
            device_id_type=MESH,
        )

    @pl.when(section < sections - 1)
    def _():
        meta_copy().start()
        for j in range(row_chunks):
            row_copy(j).start()

    for c in range(nc):
        for d in range(2):
            pltpu.make_async_remote_copy(
                src_ref=own(c),
                dst_ref=slot(c, me),
                send_sem=own_send.at[d],
                recv_sem=ring_recv.at[d, 0, c],
                device_id={"rep": towards[d]},
                device_id_type=MESH,
            ).start()
        pltpu.make_async_remote_copy(
            src_ref=own(c),
            dst_ref=slot(c, me),
            send_sem=own_send.at[2],
            recv_sem=pair_own_recv.at[c],
            device_id={"rep": partner},
            device_id_type=MESH,
        ).start()
        own_locals[c].start()

    @pl.when(section == 0)
    def _():
        meta[...] = jnp.zeros_like(meta)

        @pl.loop(0, rows // TILE)
        def _(i):
            values[pl.ds(i * TILE, TILE), :] = jnp.zeros((TILE, feature), values.dtype)

    for c in range(nq):
        bias[c] = qb_ref[:, c * CW : (c + 1) * CW]
    for c in range(nq, nc):
        bias[c] = kvb_ref[:, (c - nq) * CW : (c - nq + 1) * CW]
    keep.wait()
    for c in range(nc):
        own_locals[c].wait()

    def block_of(d, t, which):
        return rep_at(pos - t if d == 0 else pos + t, which)

    def landed(sem, c, block):
        pltpu.make_async_copy(slot(c, block), slot(c, block), sem).wait()

    def to_pair(d, t, c):
        here = slot(c, block_of(d, t, core))
        pltpu.make_async_remote_copy(
            src_ref=here,
            dst_ref=here,
            send_sem=pair_send.at[d, t - 1],
            recv_sem=pair_recv.at[d, t - 1, c],
            device_id={"rep": partner},
            device_id_type=MESH,
        ).start()

    def onward(d, t, c):
        here = slot(c, block_of(d, t, core))
        pltpu.make_async_remote_copy(
            src_ref=here,
            dst_ref=here,
            send_sem=ring_send.at[d, t - 1],
            recv_sem=ring_recv.at[d, t, c],
            device_id={"rep": towards[d]},
            device_id_type=MESH,
        ).start()

    def rebuild(j):
        @pl.when(section > 0)
        def _():
            if j == 0:
                meta_copy().wait_recv()
            row_copy(j).wait_recv()

        count = meta[3:4, 0:1]
        factor = jnp.zeros((1, 1), jnp.float32)
        for i in range(most_blk):
            live = jnp.logical_and(meta[1:2, i : i + 1] == j, count > i)
            scale = meta[2:3, i : i + 1].astype(jnp.float32) / 4096.0
            factor = factor + jnp.where(live, scale, 0.0)

        @pl.loop(0, BLK // TILE)
        def _(i):
            first = j * BLK + i * TILE
            here = pl.ds(pl.multiple_of(first, TILE), TILE)
            ids = meta[0:1, :]
            lanes = lax.broadcasted_iota(jnp.int32, ids.shape, 1)
            ids = jnp.where(lanes < meta[4:5, :], ids, -1)
            number = first + lax.broadcasted_iota(jnp.int32, (TILE, ids.shape[1]), 0)
            match = jnp.where(ids == number, 1.0, 0.0)
            hit = jnp.max(match, axis=1, keepdims=True) > 0.0
            got = values[here, :].astype(jnp.float32)
            delta = (got * factor).astype(jnp.bfloat16).astype(jnp.float32)
            mixed = jnp.where(hit, got, stored[here, :].astype(jnp.float32) + delta)
            rebuilt = mixed.astype(jnp.bfloat16)
            stored[here, :] = rebuilt
            wide = rebuilt.astype(jnp.float32)
            mean = jnp.sum(wide * wide, axis=1, keepdims=True) / feature
            scale_rows = lax.rsqrt(mean + EPSILON)
            normed[here, :] = (wide * scale_rows * gain_ref[...]).astype(jnp.bfloat16)

    def rebuilt_out(j):
        here = pl.ds(j * BLK, BLK)
        return pltpu.make_async_copy(stored.at[here, :], rebuilt_ref.at[0, here, :], out_sem.at[j])

    marks = [(j + 1) * nc // row_chunks for j in range(row_chunks)]
    marks[-1] = nc
    for t in range(1, hops):
        done = 0
        for j, mark in enumerate(marks):

            @pl.loop(done, mark)
            def _(c):
                for d in range(2):
                    landed(ring_recv.at[d, t - 1, c], c, block_of(d, t, core))
                    if t + 1 < hops:
                        onward(d, t, c)
                    else:

                        @pl.when((c < nh) if d == 0 else (c >= nc - nh))
                        def _():
                            onward(d, t, c)

                    to_pair(d, t, c)

            done = mark
            if t == 1:
                rebuild(j)
                if j > 0:
                    rebuilt_out(j - 1).start()
    rebuilt_out(row_chunks - 1).start()

    def product(c, d):
        landed(pair_own_recv.at[c], c, partner)
        for t in range(1, hops):
            for e in range(2):
                landed(pair_recv.at[e, t - 1, c], c, block_of(e, t, 1 - core))
        landed(pair_recv.at[d, hops - 1, c], c, block_of(d, hops, 1 - core))
        total = jnp.dot(normed[...], w[c], preferred_element_type=jnp.float32)
        staged[c] = (total + bias[c]).astype(jnp.bfloat16)

    def result_out(c, start):
        def go(copy):
            copy.start() if start else copy.wait()

        @pl.when(c < nq)
        def _():
            go(
                pltpu.make_async_copy(
                    staged.at[c],
                    q_ref.at[0, :, pl.ds(pl.multiple_of(c * CW, CW), CW)],
                    out_sem.at[row_chunks + c],
                )
            )

        @pl.when(c >= nq)
        def _():
            go(
                pltpu.make_async_copy(
                    staged.at[c],
                    kv_ref.at[0, :, pl.ds(pl.multiple_of((c - nq) * CW, CW), CW)],
                    out_sem.at[row_chunks + c],
                )
            )

    @pl.loop(0, nh + 1)
    def _(i):
        @pl.when(i < nh)
        def _():
            for d in range(2):
                c = i + d * nh
                landed(ring_recv.at[d, hops - 1, c], c, block_of(d, hops, core))
                to_pair(d, hops, c)

        @pl.when(i > 0)
        def _():
            for d in range(2):
                c = i - 1 + d * nh
                product(c, d)
                result_out(c, True)

    @pl.loop(0, nc)
    def _(c):
        result_out(c, False)

    for j in range(row_chunks):
        rebuilt_out(j).wait()

    def sent(sem, count):
        part = w.at[pl.ds(0, count), pl.ds(0, depth), :]
        pltpu.make_async_copy(part, part, sem).wait()

    for k in range(3):
        sent(own_send.at[k], nc)
    for d in range(2):
        for t in range(1, hops):
            sent(ring_send.at[d, t - 1], nc if t + 1 < hops else nh)
            sent(pair_send.at[d, t - 1], nc)
        sent(pair_send.at[d, hops - 1], nh)

    @pl.when(section < sections - 1)
    def _():
        meta_copy().wait_send()
        for j in range(row_chunks):
            row_copy(j).wait_send()


def body(
    cache,
    payload,
    block_ids,
    block_counts,
    block_scales,
    refresh_ids,
    refresh_counts,
    norm_gain,
    query_weight,
    query_bias,
    kv_weight,
    kv_bias,
):
    sections = lax.axis_size("section")
    reps = lax.axis_size("rep")
    rows, feature = cache.shape[1:]
    depth = query_weight.shape[1]
    queries = query_weight.shape[2]
    keys = kv_weight.shape[2]
    most_blk = block_ids.shape[2]
    width = refresh_ids.shape[2]
    nc = (queries + keys) // CW
    hops = reps // 4
    row_chunks = rows // BLK

    def line(values):
        return jnp.pad(values[0], ((0, 0), (0, width - values.shape[2])))

    meta = jnp.concatenate(
        [
            refresh_ids[0],
            line(block_ids),
            line(block_scales),
            jnp.broadcast_to(block_counts, (1, width)),
            jnp.broadcast_to(refresh_counts, (4, width)),
        ],
        axis=0,
    )
    vmem = pl.BlockSpec(memory_space=pltpu.VMEM)
    anywhere = pl.BlockSpec(memory_space=pl.ANY)
    dma = pltpu.SemaphoreType.DMA
    return pl.pallas_call(
        functools.partial(kernel, sections, reps, most_blk),
        out_shape=(
            jax.ShapeDtypeStruct(cache.shape, cache.dtype),
            jax.ShapeDtypeStruct((1, rows, queries), cache.dtype),
            jax.ShapeDtypeStruct((1, rows, keys), cache.dtype),
        ),
        in_specs=[vmem, anywhere, anywhere, vmem, anywhere, vmem, anywhere, vmem],
        out_specs=(anywhere, anywhere, anywhere),
        scratch_shapes=[
            pltpu.VMEM((nc, reps * depth, CW), jnp.bfloat16),
            pltpu.VMEM((rows, feature), jnp.bfloat16),
            pltpu.VMEM((rows, feature), jnp.bfloat16),
            pltpu.VMEM((rows, feature), jnp.bfloat16),
            pltpu.VMEM((nc, rows, CW), jnp.bfloat16),
            pltpu.VMEM((nc, 1, CW), jnp.float32),
            pltpu.VMEM((8, width), jnp.int32),
            dma((nc,)),
            dma,
            dma((row_chunks + 1,)),
            dma((row_chunks + 1,)),
            dma((3,)),
            dma((nc,)),
            dma((2, hops)),
            dma((2, hops, nc)),
            dma((2, hops)),
            dma((2, hops, nc)),
            dma((row_chunks + nc,)),
        ],
        compiler_params=pltpu.CompilerParams(
            collective_id=0, has_side_effects=True, vmem_limit_bytes=60 * 1024 * 1024
        ),
    )(meta, payload, cache, norm_gain, query_weight, query_bias, kv_weight, kv_bias)


def solution(mesh):
    in_specs = (
        P("section", "rep", None),
        P("section", "rep", None),
        P("section", "rep", None),
        P("section", "rep"),
        P("section", "rep", None),
        P("section", "rep", None),
        P("section", "rep"),
        P("section", None),
        P("section", "rep", None),
        P("section", None),
        P("section", "rep", None),
        P("section", None),
    )
    out_specs = (P("section", "rep", None), P("section", "rep", None), P("section", "rep", None))
    return jax.shard_map(body, mesh=mesh, in_specs=in_specs, out_specs=out_specs, check_vma=False)
```

```python
import functools

import jax
import jax.numpy as jnp
from jax import lax
from jax.experimental import pallas as pl
from jax.experimental.pallas import tpu as pltpu
from jax.sharding import PartitionSpec as P

BLK = 128
CW = 256
TILE = 16
EPSILON = 1e-06
MESH = pl.DeviceIdType.MESH


def chip_at(pos, chips):
    half = chips // 2
    back = pos // half
    return pos + back * (half + chips - 1 - 2 * pos)


def kernel(
    sections,
    reps,
    most_blk,
    lists_ref,
    payload_ref,
    cache_ref,
    gain_ref,
    qw_ref,
    qb_ref,
    kvw_ref,
    kvb_ref,
    rebuilt_ref,
    q_ref,
    kv_ref,
    w,
    values,
    normed,
    sums,
    bias,
    lists,
    local_sem,
    keep_sem,
    row_send,
    row_recv,
    own_send,
    pair_own_recv,
    ring_send,
    ring_recv,
    pair_send,
    pair_recv,
):
    chips = reps // 2
    hops = chips // 2
    depth = qw_ref.shape[1]
    rows = payload_ref.shape[1]
    feature = payload_ref.shape[2]
    nq = qw_ref.shape[2] // CW
    nc = nq + kvw_ref.shape[2] // CW
    nh = nc // 2
    row_chunks = rows // BLK

    section = lax.axis_index("section")
    me = lax.axis_index("rep")
    core = me % 2
    chip = me // 2
    pos = chip + (chip // hops) * (hops + chips - 1 - 2 * chip)
    partner = 2 * chip + (1 - core)

    def rep_at(place, which):
        return 2 * chip_at((place + chips) % chips, chips) + which

    towards = (rep_at(pos + 1, core), rep_at(pos - 1, core))

    barrier = pltpu.get_barrier_semaphore()
    for other in (partner,) + towards:
        pl.semaphore_signal(barrier, 1, device_id={"rep": other}, device_id_type=MESH)

    @pl.when(section > 0)
    def _():
        pl.semaphore_signal(
            barrier, 1, device_id={"section": section - 1}, device_id_type=MESH
        )

    @pl.when(section < sections - 1)
    def _():
        pl.semaphore_signal(
            barrier, 1, device_id={"section": section + 1}, device_id_type=MESH
        )

    def own(c):
        if c < nq:
            return qw_ref.at[0, :, pl.ds(c * CW, CW)]
        return kvw_ref.at[0, :, pl.ds((c - nq) * CW, CW)]

    def slot(c, block):
        return w.at[c, pl.ds(pl.multiple_of(block * depth, depth), depth), :]

    keep = pltpu.make_async_copy(cache_ref, rebuilt_ref, keep_sem)
    keep.start()
    own_locals = [
        pltpu.make_async_copy(own(c), slot(c, me), local_sem.at[c]) for c in range(nc)
    ]

    sides = (section + sections - 1) // sections + (2 * sections - 2 - section) // sections
    pl.semaphore_wait(barrier, 3 + sides)

    def list_copy(i):
        return pltpu.make_async_remote_copy(
            src_ref=lists_ref[i],
            dst_ref=lists[i],
            send_sem=row_send.at[row_chunks + i],
            recv_sem=row_recv.at[row_chunks + i],
            device_id={"section": section + 1},
            device_id_type=MESH,
        )

    def row_copy(j):
        return pltpu.make_async_remote_copy(
            src_ref=payload_ref.at[0, pl.ds(j * BLK, BLK), :],
            dst_ref=values.at[pl.ds(j * BLK, BLK), :],
            send_sem=row_send.at[j],
            recv_sem=row_recv.at[j],
            device_id={"section": section + 1},
            device_id_type=MESH,
        )

    @pl.when(section < sections - 1)
    def _():
        for i in range(len(lists)):
            list_copy(i).start()
        for j in range(row_chunks):
            row_copy(j).start()

    for c in range(nc):
        for d in range(2):
            pltpu.make_async_remote_copy(
                src_ref=own(c),
                dst_ref=slot(c, me),
                send_sem=own_send.at[d],
                recv_sem=ring_recv.at[d, 0, c],
                device_id={"rep": towards[d]},
                device_id_type=MESH,
            ).start()
        pltpu.make_async_remote_copy(
            src_ref=own(c),
            dst_ref=slot(c, me),
            send_sem=own_send.at[2],
            recv_sem=pair_own_recv.at[c],
            device_id={"rep": partner},
            device_id_type=MESH,
        ).start()
        own_locals[c].start()

    @pl.when(section == 0)
    def _():
        for ref in lists:
            ref[...] = jnp.zeros_like(ref)

        @pl.loop(0, rows // TILE)
        def _(i):
            values[pl.ds(i * TILE, TILE), :] = jnp.zeros((TILE, feature), values.dtype)

    for c in range(nq):
        bias[c] = qb_ref[:, c * CW : (c + 1) * CW]
    for c in range(nq, nc):
        bias[c] = kvb_ref[:, (c - nq) * CW : (c - nq + 1) * CW]
    keep.wait()
    for c in range(nc):
        own_locals[c].wait()

    def block_of(d, t, which):
        return rep_at(pos - t if d == 0 else pos + t, which)

    def landed(sem, c, block):
        pltpu.make_async_copy(slot(c, block), slot(c, block), sem).wait()

    def to_pair(d, t, c):
        here = slot(c, block_of(d, t, core))
        pltpu.make_async_remote_copy(
            src_ref=here,
            dst_ref=here,
            send_sem=pair_send.at[d, t - 1],
            recv_sem=pair_recv.at[d, t - 1, c],
            device_id={"rep": partner},
            device_id_type=MESH,
        ).start()

    def onward(d, t, c):
        here = slot(c, block_of(d, t, core))
        pltpu.make_async_remote_copy(
            src_ref=here,
            dst_ref=here,
            send_sem=ring_send.at[d, t - 1],
            recv_sem=ring_recv.at[d, t, c],
            device_id={"rep": towards[d]},
            device_id_type=MESH,
        ).start()

    def rebuild(j):
        @pl.when(section > 0)
        def _():
            if j == 0:
                for i in range(len(lists)):
                    list_copy(i).wait_recv()
            row_copy(j).wait_recv()

        got_rows, got_ids, got_scales, got_counts, got_rcounts = lists
        count = got_counts[...]
        factor = jnp.zeros((1, 1), jnp.float32)
        for i in range(most_blk):
            live = jnp.logical_and(got_ids[:, i : i + 1] == j, count > i)
            scale = got_scales[:, i : i + 1].astype(jnp.float32) / 4096.0
            factor = factor + jnp.where(live, scale, 0.0)

        @pl.loop(0, BLK // TILE)
        def _(i):
            first = j * BLK + i * TILE
            here = pl.ds(pl.multiple_of(first, TILE), TILE)
            ids = got_rows[...]
            lanes = lax.broadcasted_iota(jnp.int32, ids.shape, 1)
            ids = jnp.where(lanes < got_rcounts[...], ids, -1)
            number = first + lax.broadcasted_iota(jnp.int32, (TILE, ids.shape[1]), 0)
            match = jnp.where(ids == number, 1.0, 0.0)
            hit = jnp.max(match, axis=1, keepdims=True) > 0.0
            got = values[here, :].astype(jnp.float32)
            delta = (got * factor).astype(jnp.bfloat16).astype(jnp.float32)
            mixed = jnp.where(hit, got, rebuilt_ref[0, here, :].astype(jnp.float32) + delta)
            rebuilt = mixed.astype(jnp.bfloat16)
            rebuilt_ref[0, here, :] = rebuilt
            wide = rebuilt.astype(jnp.float32)
            mean = jnp.sum(wide * wide, axis=1, keepdims=True) / feature
            scale_rows = lax.rsqrt(mean + EPSILON)
            result = (wide * scale_rows * gain_ref[...]).astype(jnp.bfloat16)
            for k in range(chips):
                normed[k, here, :] = result[:, 2 * depth * k : 2 * depth * (k + 1)]

    marks = [(j + 1) * nc // row_chunks for j in range(row_chunks)]
    marks[-1] = nc
    for t in range(1, hops):
        done = 0
        for j, mark in enumerate(marks):

            @pl.loop(done, mark)
            def _(c):
                for d in range(2):
                    landed(ring_recv.at[d, t - 1, c], c, block_of(d, t, core))
                    if t + 1 < hops:
                        onward(d, t, c)
                    else:

                        @pl.when((c < nh) if d == 0 else (c >= nc - nh))
                        def _():
                            onward(d, t, c)

                    to_pair(d, t, c)

            done = mark
            if t == 1:
                rebuild(j)

    far = chip_at((pos + hops) % chips, chips)
    wide_depth = 2 * depth

    def term(c, which):
        rows_here = pl.ds(pl.multiple_of(which * wide_depth, wide_depth), wide_depth)
        return jnp.dot(normed[which], w[c, rows_here, :], preferred_element_type=jnp.float32)

    def partial(i):
        for d in range(2):
            c = i + d * nh
            landed(pair_own_recv.at[c], c, partner)
            for t in range(1, hops):
                for e in range(2):
                    landed(pair_recv.at[e, t - 1, c], c, block_of(e, t, 1 - core))
            total = bias[c]
            for step in range(1, chips):
                total = total + term(c, (far + step) % chips)
            sums[i % 2, d] = total

    def finish(i):
        for d in range(2):
            c = i + d * nh
            landed(pair_recv.at[d, hops - 1, c], c, block_of(d, hops, 1 - core))
            result = (sums[i % 2, d] + term(c, far)).astype(jnp.bfloat16)

            @pl.when(c < nq)
            def _():
                q_ref[0, :, pl.ds(pl.multiple_of(c * CW, CW), CW)] = result

            @pl.when(c >= nq)
            def _():
                kv_ref[0, :, pl.ds(pl.multiple_of((c - nq) * CW, CW), CW)] = result

    partial(0)

    @pl.loop(0, nh)
    def _(i):
        for d in range(2):
            c = i + d * nh
            landed(ring_recv.at[d, hops - 1, c], c, block_of(d, hops, core))
            to_pair(d, hops, c)

        @pl.when(i + 1 < nh)
        def _():
            partial(i + 1)

        finish(i)

    def sent(sem, count):
        part = w.at[pl.ds(0, count), pl.ds(0, depth), :]
        pltpu.make_async_copy(part, part, sem).wait()

    for k in range(3):
        sent(own_send.at[k], nc)
    for d in range(2):
        for t in range(1, hops):
            sent(ring_send.at[d, t - 1], nc if t + 1 < hops else nh)
            sent(pair_send.at[d, t - 1], nc)
        sent(pair_send.at[d, hops - 1], nh)

    @pl.when(section < sections - 1)
    def _():
        for i in range(len(lists)):
            list_copy(i).wait_send()
        for j in range(row_chunks):
            row_copy(j).wait_send()


def body(
    cache,
    payload,
    block_ids,
    block_counts,
    block_scales,
    refresh_ids,
    refresh_counts,
    norm_gain,
    query_weight,
    query_bias,
    kv_weight,
    kv_bias,
):
    sections = lax.axis_size("section")
    reps = lax.axis_size("rep")
    rows, feature = cache.shape[1:]
    depth = query_weight.shape[1]
    queries = query_weight.shape[2]
    keys = kv_weight.shape[2]
    most_blk = block_ids.shape[2]
    nc = (queries + keys) // CW
    hops = reps // 4
    row_chunks = rows // BLK

    lists = (refresh_ids[0], block_ids[0], block_scales[0], block_counts, refresh_counts)
    vmem = pl.BlockSpec(memory_space=pltpu.VMEM)
    anywhere = pl.BlockSpec(memory_space=pltpu.HBM)
    dma = pltpu.SemaphoreType.DMA
    return pl.pallas_call(
        functools.partial(kernel, sections, reps, most_blk),
        out_shape=(
            pltpu.VMEM(cache.shape, cache.dtype),
            pltpu.VMEM((1, rows, queries), cache.dtype),
            pltpu.VMEM((1, rows, keys), cache.dtype),
        ),
        in_specs=[(anywhere,) * len(lists), anywhere, anywhere, vmem, anywhere, vmem, anywhere, vmem],
        out_specs=(vmem, vmem, vmem),
        scratch_shapes=[
            pltpu.VMEM((nc, reps * depth, CW), jnp.bfloat16),
            pltpu.VMEM((rows, feature), jnp.bfloat16),
            pltpu.VMEM((reps // 2, rows, 2 * depth), jnp.bfloat16),
            pltpu.VMEM((2, 2, rows, CW), jnp.float32),
            pltpu.VMEM((nc, 1, CW), jnp.float32),
            tuple(pltpu.VMEM(x.shape, x.dtype) for x in lists),
            dma((nc,)),
            dma,
            dma((row_chunks + len(lists),)),
            dma((row_chunks + len(lists),)),
            dma((3,)),
            dma((nc,)),
            dma((2, hops)),
            dma((2, hops, nc)),
            dma((2, hops)),
            dma((2, hops, nc)),
        ],
        compiler_params=pltpu.CompilerParams(
            collective_id=0, has_side_effects=True, vmem_limit_bytes=111 * 512 * 1024
        ),
    )(lists, payload, cache, norm_gain, query_weight, query_bias, kv_weight, kv_bias)


def solution(mesh):
    in_specs = (
        P("section", "rep", None),
        P("section", "rep", None),
        P("section", "rep", None),
        P("section", "rep"),
        P("section", "rep", None),
        P("section", "rep", None),
        P("section", "rep"),
        P("section", None),
        P("section", "rep", None),
        P("section", None),
        P("section", "rep", None),
        P("section", None),
    )
    out_specs = (P("section", "rep", None), P("section", "rep", None), P("section", "rep", None))
    return jax.shard_map(body, mesh=mesh, in_specs=in_specs, out_specs=out_specs, check_vma=False)
```

```python
import functools

import jax
import jax.numpy as jnp
from jax import lax
from jax.experimental import pallas as pl
from jax.experimental.pallas import tpu as pltpu
from jax.sharding import PartitionSpec as P

BLK = 128
CW = 256
TILE = 16
EPSILON = 1e-06
MESH = pl.DeviceIdType.MESH


def chip_at(pos, chips):
    half = chips // 2
    back = pos // half
    return pos + back * (half + chips - 1 - 2 * pos)


def kernel(
    sections,
    reps,
    most_blk,
    lists_ref,
    payload_ref,
    cache_ref,
    gain_ref,
    qw_ref,
    qb_ref,
    kvw_ref,
    kvb_ref,
    rebuilt_ref,
    q_ref,
    kv_ref,
    w,
    values,
    normed,
    sums,
    bias,
    lists,
    local_sem,
    keep_sem,
    row_send,
    row_recv,
    own_send,
    pair_own_recv,
    ring_send,
    ring_recv,
    pair_send,
    pair_recv,
):
    chips = reps // 2
    hops = chips // 2
    depth = qw_ref.shape[1]
    rows = payload_ref.shape[1]
    feature = payload_ref.shape[2]
    nq = qw_ref.shape[2] // CW
    nc = nq + kvw_ref.shape[2] // CW
    nh = nc // 2
    row_chunks = rows // BLK

    section = lax.axis_index("section")
    me = lax.axis_index("rep")
    core = me % 2
    chip = me // 2
    pos = chip + (chip // hops) * (hops + chips - 1 - 2 * chip)
    partner = 2 * chip + (1 - core)

    def rep_at(place, which):
        return 2 * chip_at((place + chips) % chips, chips) + which

    towards = (rep_at(pos + 1, core), rep_at(pos - 1, core))

    barrier = pltpu.get_barrier_semaphore()
    for other in (partner,) + towards:
        pl.semaphore_signal(barrier, 1, device_id={"rep": other}, device_id_type=MESH)

    @pl.when(section > 0)
    def _():
        pl.semaphore_signal(
            barrier, 1, device_id={"section": section - 1}, device_id_type=MESH
        )

    @pl.when(section < sections - 1)
    def _():
        pl.semaphore_signal(
            barrier, 1, device_id={"section": section + 1}, device_id_type=MESH
        )

    def own(c):
        if c < nq:
            return qw_ref.at[0, :, pl.ds(c * CW, CW)]
        return kvw_ref.at[0, :, pl.ds((c - nq) * CW, CW)]

    def slot(c, block):
        return w.at[c, pl.ds(pl.multiple_of(block * depth, depth), depth), :]

    keep = pltpu.make_async_copy(cache_ref, rebuilt_ref, keep_sem)
    keep.start()
    own_locals = [
        pltpu.make_async_copy(own(c), slot(c, me), local_sem.at[c]) for c in range(nc)
    ]

    sides = (section + sections - 1) // sections + (2 * sections - 2 - section) // sections
    pl.semaphore_wait(barrier, 3 + sides)

    def list_copy(i):
        return pltpu.make_async_remote_copy(
            src_ref=lists_ref[i],
            dst_ref=lists[i],
            send_sem=row_send.at[row_chunks + i],
            recv_sem=row_recv.at[row_chunks + i],
            device_id={"section": section + 1},
            device_id_type=MESH,
        )

    def row_copy(j):
        return pltpu.make_async_remote_copy(
            src_ref=payload_ref.at[0, pl.ds(j * BLK, BLK), :],
            dst_ref=values.at[pl.ds(j * BLK, BLK), :],
            send_sem=row_send.at[j],
            recv_sem=row_recv.at[j],
            device_id={"section": section + 1},
            device_id_type=MESH,
        )

    @pl.when(section < sections - 1)
    def _():
        for i in range(len(lists)):
            list_copy(i).start()
        for j in range(row_chunks):
            row_copy(j).start()

    for c in range(nc):
        for d in range(2):
            pltpu.make_async_remote_copy(
                src_ref=own(c),
                dst_ref=slot(c, me),
                send_sem=own_send.at[d],
                recv_sem=ring_recv.at[d, 0, c],
                device_id={"rep": towards[d]},
                device_id_type=MESH,
            ).start()
        pltpu.make_async_remote_copy(
            src_ref=own(c),
            dst_ref=slot(c, me),
            send_sem=own_send.at[2],
            recv_sem=pair_own_recv.at[c],
            device_id={"rep": partner},
            device_id_type=MESH,
        ).start()
        own_locals[c].start()

    @pl.when(section == 0)
    def _():
        for ref in lists:
            ref[...] = jnp.zeros_like(ref)

        @pl.loop(0, rows // TILE)
        def _(i):
            values[pl.ds(i * TILE, TILE), :] = jnp.zeros((TILE, feature), values.dtype)

    for c in range(nq):
        bias[c] = qb_ref[:, c * CW : (c + 1) * CW]
    for c in range(nq, nc):
        bias[c] = kvb_ref[:, (c - nq) * CW : (c - nq + 1) * CW]
    keep.wait()
    for c in range(nc):
        own_locals[c].wait()

    def block_of(d, t, which):
        return rep_at(pos - t if d == 0 else pos + t, which)

    def landed(sem, c, block):
        pltpu.make_async_copy(slot(c, block), slot(c, block), sem).wait()

    def to_pair(d, t, c):
        here = slot(c, block_of(d, t, core))
        pltpu.make_async_remote_copy(
            src_ref=here,
            dst_ref=here,
            send_sem=pair_send.at[d, t - 1],
            recv_sem=pair_recv.at[d, t - 1, c],
            device_id={"rep": partner},
            device_id_type=MESH,
        ).start()

    def onward(d, t, c):
        here = slot(c, block_of(d, t, core))
        pltpu.make_async_remote_copy(
            src_ref=here,
            dst_ref=here,
            send_sem=ring_send.at[d, t - 1],
            recv_sem=ring_recv.at[d, t, c],
            device_id={"rep": towards[d]},
            device_id_type=MESH,
        ).start()

    def rebuild(j):
        @pl.when(section > 0)
        def _():
            if j == 0:
                for i in range(len(lists)):
                    list_copy(i).wait_recv()
            row_copy(j).wait_recv()

        got_rows, got_ids, got_scales, got_counts, got_rcounts = lists
        count = got_counts[...]
        factor = jnp.zeros((1, 1), jnp.float32)
        for i in range(most_blk):
            live = jnp.logical_and(got_ids[:, i : i + 1] == j, count > i)
            scale = got_scales[:, i : i + 1].astype(jnp.float32) / 4096.0
            factor = factor + jnp.where(live, scale, 0.0)

        @pl.loop(0, BLK // TILE)
        def _(i):
            first = j * BLK + i * TILE
            here = pl.ds(pl.multiple_of(first, TILE), TILE)
            ids = got_rows[...]
            lanes = lax.broadcasted_iota(jnp.int32, ids.shape, 1)
            ids = jnp.where(lanes < got_rcounts[...], ids, -1)
            number = first + lax.broadcasted_iota(jnp.int32, (TILE, ids.shape[1]), 0)
            match = jnp.where(ids == number, 1.0, 0.0)
            hit = jnp.max(match, axis=1, keepdims=True) > 0.0
            got = values[here, :].astype(jnp.float32)
            delta = (got * factor).astype(jnp.bfloat16).astype(jnp.float32)
            mixed = jnp.where(hit, got, rebuilt_ref[0, here, :].astype(jnp.float32) + delta)
            rebuilt = mixed.astype(jnp.bfloat16)
            rebuilt_ref[0, here, :] = rebuilt
            wide = rebuilt.astype(jnp.float32)
            mean = jnp.sum(wide * wide, axis=1, keepdims=True) / feature
            scale_rows = lax.rsqrt(mean + EPSILON)
            result = (wide * scale_rows * gain_ref[...]).astype(jnp.bfloat16)
            for k in range(chips):
                normed[k, here, :] = result[:, 2 * depth * k : 2 * depth * (k + 1)]

    marks = [(j + 1) * nc // row_chunks for j in range(row_chunks)]
    marks[-1] = nc
    for t in range(1, hops):
        done = 0
        for j, mark in enumerate(marks):

            @pl.loop(done, mark)
            def _(c):
                for d in range(2):
                    landed(ring_recv.at[d, t - 1, c], c, block_of(d, t, core))
                    if t + 1 < hops:
                        onward(d, t, c)
                    else:

                        @pl.when((c < nh) if d == 0 else (c >= nc - nh))
                        def _():
                            onward(d, t, c)

                    to_pair(d, t, c)

            done = mark
            if t == 1:
                rebuild(j)

    far = chip_at((pos + hops) % chips, chips)
    wide_depth = 2 * depth

    def term(c, which):
        rows_here = pl.ds(pl.multiple_of(which * wide_depth, wide_depth), wide_depth)
        return jnp.dot(normed[which], w[c, rows_here, :], preferred_element_type=jnp.float32)

    def partial(i):
        for d in range(2):
            c = i + d * nh
            landed(pair_own_recv.at[c], c, partner)
            for t in range(1, hops):
                for e in range(2):
                    landed(pair_recv.at[e, t - 1, c], c, block_of(e, t, 1 - core))
            total = bias[c]
            for step in range(1, chips):
                total = total + term(c, (far + step) % chips)
            sums[i % 2, d] = total

    def finish(i):
        for d in range(2):
            c = i + d * nh
            landed(pair_recv.at[d, hops - 1, c], c, block_of(d, hops, 1 - core))
            result = (sums[i % 2, d] + term(c, far)).astype(jnp.bfloat16)

            @pl.when(c < nq)
            def _():
                q_ref[0, :, pl.ds(pl.multiple_of(c * CW, CW), CW)] = result

            @pl.when(c >= nq)
            def _():
                kv_ref[0, :, pl.ds(pl.multiple_of((c - nq) * CW, CW), CW)] = result

    partial(0)

    @pl.loop(0, nh)
    def _(i):
        for d in range(2):
            c = i + d * nh
            landed(ring_recv.at[d, hops - 1, c], c, block_of(d, hops, core))
            to_pair(d, hops, c)

        @pl.when(i + 1 < nh)
        def _():
            partial(i + 1)

        finish(i)

    def sent(sem, count):
        part = w.at[pl.ds(0, count), pl.ds(0, depth), :]
        pltpu.make_async_copy(part, part, sem).wait()

    for k in range(3):
        sent(own_send.at[k], nc)
    for d in range(2):
        for t in range(1, hops):
            sent(ring_send.at[d, t - 1], nc if t + 1 < hops else nh)
            sent(pair_send.at[d, t - 1], nc)
        sent(pair_send.at[d, hops - 1], nh)

    @pl.when(section < sections - 1)
    def _():
        for i in range(len(lists)):
            list_copy(i).wait_send()
        for j in range(row_chunks):
            row_copy(j).wait_send()


def put_out(parts, *refs):
    count = (len(refs) - 1) // 2
    sem = refs[-1]
    copies = []
    for k in range(count):
        source, target = refs[k], refs[count + k]
        step = source.shape[1] // parts
        for j in range(parts):
            here = pl.ds(j * step, step)
            copies.append(
                pltpu.make_async_copy(
                    source.at[:, here, :], target.at[:, here, :], sem.at[k * parts + j]
                )
            )
    for copy in copies:
        copy.start()
    for copy in copies:
        copy.wait()


def body(
    cache,
    payload,
    block_ids,
    block_counts,
    block_scales,
    refresh_ids,
    refresh_counts,
    norm_gain,
    query_weight,
    query_bias,
    kv_weight,
    kv_bias,
):
    sections = lax.axis_size("section")
    reps = lax.axis_size("rep")
    rows, feature = cache.shape[1:]
    depth = query_weight.shape[1]
    queries = query_weight.shape[2]
    keys = kv_weight.shape[2]
    most_blk = block_ids.shape[2]
    nc = (queries + keys) // CW
    hops = reps // 4
    row_chunks = rows // BLK

    lists = (refresh_ids[0], block_ids[0], block_scales[0], block_counts, refresh_counts)
    vmem = pl.BlockSpec(memory_space=pltpu.VMEM)
    anywhere = pl.BlockSpec(memory_space=pltpu.HBM)
    dma = pltpu.SemaphoreType.DMA
    results = pl.pallas_call(
        functools.partial(kernel, sections, reps, most_blk),
        out_shape=(
            pltpu.VMEM(cache.shape, cache.dtype),
            pltpu.VMEM((1, rows, queries), cache.dtype),
            pltpu.VMEM((1, rows, keys), cache.dtype),
        ),
        in_specs=[(anywhere,) * len(lists), anywhere, anywhere, vmem, anywhere, vmem, anywhere, vmem],
        out_specs=(vmem, vmem, vmem),
        scratch_shapes=[
            pltpu.VMEM((nc, reps * depth, CW), jnp.bfloat16),
            pltpu.VMEM((rows, feature), jnp.bfloat16),
            pltpu.VMEM((reps // 2, rows, 2 * depth), jnp.bfloat16),
            pltpu.VMEM((2, 2, rows, CW), jnp.float32),
            pltpu.VMEM((nc, 1, CW), jnp.float32),
            tuple(pltpu.VMEM(x.shape, x.dtype) for x in lists),
            dma((nc,)),
            dma,
            dma((row_chunks + len(lists),)),
            dma((row_chunks + len(lists),)),
            dma((3,)),
            dma((nc,)),
            dma((2, hops)),
            dma((2, hops, nc)),
            dma((2, hops)),
            dma((2, hops, nc)),
        ],
        compiler_params=pltpu.CompilerParams(
            collective_id=0, has_side_effects=True, vmem_limit_bytes=111 * 512 * 1024
        ),
    )(lists, payload, cache, norm_gain, query_weight, query_bias, kv_weight, kv_bias)
    parts = row_chunks
    return tuple(
        pl.pallas_call(
            functools.partial(put_out, parts),
            out_shape=tuple(pltpu.HBM(x.shape, x.dtype) for x in results),
            in_specs=[vmem] * len(results),
            out_specs=(anywhere,) * len(results),
            scratch_shapes=[dma((parts * len(results),))],
            compiler_params=pltpu.CompilerParams(vmem_limit_bytes=1024 * 1024),
        )(*results)
    )


def solution(mesh):
    in_specs = (
        P("section", "rep", None),
        P("section", "rep", None),
        P("section", "rep", None),
        P("section", "rep"),
        P("section", "rep", None),
        P("section", "rep", None),
        P("section", "rep"),
        P("section", None),
        P("section", "rep", None),
        P("section", None),
        P("section", "rep", None),
        P("section", None),
    )
    out_specs = (P("section", "rep", None), P("section", "rep", None), P("section", "rep", None))
    return jax.shard_map(body, mesh=mesh, in_specs=in_specs, out_specs=out_specs, check_vma=False)
```
